128 devices in a mesh: vocab: 32 (over x, z, core), group: 4 (over y).
Axes of the slice: x: 4, y: 4, z: 4, core: 2. Of those that a mesh axis runs over, the one named last changes fastest.
Arguments:
- hidden_states: bfloat16 [2048, 4096], P(('group', 'vocab')), parts along dimension 0, may hold values from -32 to 32
- head_weight: bfloat16 [4096, 77824], P(None, 'vocab'), may hold values from -1 to 1
- pick_index: int32 [2048, 64], P('group'), parts along dimension 0, may hold values from 0 to 77823, as said below
- owner_order: int32 [2048], P('group'), parts along dimension 0, may hold values from 0 to 511, each once
Outputs:
- token_logprobs: float32 [2048, 64], P(('group', 'vocab')), parts along dimension 0
- token_logtotal: float32 [2048], P(('group', 'vocab')), parts along dimension 0
The draws below stay inside these ranges and needn't reach their ends.
There are 4 independent parts, one for each index of `group`. The reference program is written for one: setup_inputs(seed, part) draws one part's arguments, and reference() takes and returns one part's arrays. A program takes and returns all parts, laid end to end along the dimension named above; an argument that names none is the same for every part. Nothing has to cross between parts.
Inputs may be any that keep to these rules, and one draw needn't show every extreme that they name: `pick_index`: each row holds 64 distinct vocabulary entries. `owner_order`: each token appears once.
All inputs are finite; a program needn't handle non-finite values.
Results may differ from the reference program's by a relative error of at most 0.0003.
Values may be sent and summed in bfloat16 or wider, within the bound.
No kernel may reach another device: no remote copies, remote signals or barrier semaphores. Data moves between devices by JAX's collectives and lax.ppermute only.
A program may use at most 128 MiB of HBM per device.

```python
import math
import jax
import jax.numpy as jnp

D = 4096
K = 64
TOKENS = 512
VOCAB = 77824


def weight_column(key, column):
    column_key = jax.random.fold_in(jax.random.fold_in(key, 7), column)
    values = jnp.clip(jax.random.normal(column_key, (D,), jnp.float32), -6.0, 6.0)
    factor = jnp.exp(jax.random.uniform(jax.random.fold_in(column_key, 1), (), jnp.float32, math.log(0.7), math.log(1.4)))
    position = column.astype(jnp.float32) / VOCAB
    scale = 3.0 * jnp.exp(0.13 * position) * factor
    return values * scale / math.sqrt(D)


def draw_head_weight(key, part):
    columns = jax.vmap(lambda column: weight_column(key, column))(jnp.arange(VOCAB, dtype=jnp.int32))
    result = columns.T
    return jnp.clip(result, -1.0, 1.0).astype(jnp.bfloat16)


def draw_hidden_states(key, part):
    base_key = jax.random.fold_in(key, 11)
    result = jnp.clip(jax.random.normal(base_key, (TOKENS, D), jnp.float32), -6.0, 6.0)
    return jnp.clip(result, -32.0, 32.0).astype(jnp.bfloat16)


def draw_pick_index(key, part):
    base_key = jax.random.fold_in(key, 21)
    raw_draw = jax.random.randint(base_key, (TOKENS, K), 0, VOCAB - K + 1)
    spread = jnp.sort(raw_draw, axis=1) + jnp.arange(K, dtype=jnp.int32)[None, :]
    scores = jax.random.randint(jax.random.fold_in(base_key, 1), (TOKENS, K), 0, 1 << 20) * K + jnp.arange(K, dtype=jnp.int32)[None, :]
    shuffle = jnp.argsort(scores, axis=1, stable=True)
    return jnp.take_along_axis(spread, shuffle, axis=1).astype(jnp.int32)


def setup_inputs(seed: int = 0, part: int = 0) -> dict:
    streams_of = jax.random.split(jax.random.key(seed), 5)
    own_keys = jax.random.split(jax.random.fold_in(streams_of[4], part), 5)
    hidden_states = draw_hidden_states(jax.random.fold_in(jax.random.fold_in(streams_of[4], part), 71), part)
    head_weight = draw_head_weight(jax.random.fold_in(streams_of[4], 71), part)
    pick_index = draw_pick_index(jax.random.fold_in(jax.random.fold_in(streams_of[4], part), 71), part)
    owner_order = jax.random.permutation(own_keys[3], TOKENS).astype(jnp.int32)
    return {"hidden_states": hidden_states, "head_weight": head_weight, "pick_index": pick_index, "owner_order": owner_order}


def reference(hidden_states, head_weight, pick_index, owner_order):
    logits = jnp.dot(hidden_states, head_weight, preferred_element_type=jnp.float32)
    row_max = jnp.max(logits, axis=1)
    log_total = row_max + jnp.log(jnp.sum(jnp.exp(logits - row_max[:, None]), axis=1))
    picked = jnp.take_along_axis(logits, pick_index, axis=1) - log_total[:, None]
    return picked[owner_order], log_total[owner_order]
```

```python
import functools

import jax
import jax.numpy as jnp
from jax import lax
from jax.experimental import pallas as pl
from jax.experimental.pallas import tpu as pltpu
from jax.sharding import PartitionSpec as P

LANES = 128
ROWS = 8


def pick_kernel(order_ref, logits_ref, index_ref, out_ref, held_ref, *, unroll):
    tokens, width = logits_ref.shape
    picks = index_ref.shape[1]
    lane = lax.broadcasted_iota(jnp.int32, (ROWS, LANES), 1)

    def block(b, _):
        rows = pl.ds(pl.multiple_of(b * ROWS, ROWS), ROWS)
        local = index_ref[rows, :]
        tile = lax.shift_right_arithmetic(local, 7)
        at = lax.bitwise_and(local, LANES - 1)
        top = jnp.max(logits_ref[rows, :], axis=1, keepdims=True)
        total = jnp.sum(jnp.exp(logits_ref[rows, :] - top), axis=1, keepdims=True)
        found = jnp.zeros((ROWS, LANES), jnp.float32)
        for j in range(width // LANES):
            part = logits_ref[rows, j * LANES : (j + 1) * LANES]
            seen = jnp.take_along_axis(part, at, axis=1, mode="promise_in_bounds")
            found = jnp.where(tile == j, seen, found)
        found = jnp.where(lane == LANES - 2, top, found)
        found = jnp.where(lane == LANES - 1, total, found)
        held_ref[rows, :] = found
        return 0

    lax.fori_loop(0, tokens // ROWS, block, 0)

    def move(b, _):
        for i in range(unroll):
            r = b * unroll + i
            out_ref[pl.ds(r, 1), :] = held_ref[pl.ds(order_ref[r], 1), :]
        return 0

    lax.fori_loop(0, tokens // unroll, move, 0)


def picked_and_stats(logits, local_index, owner_order):
    tokens, width = logits.shape
    spare = LANES - local_index.shape[1]
    index = jnp.pad(local_index, ((0, 0), (0, spare)), constant_values=-1)
    return pl.pallas_call(
        functools.partial(pick_kernel, unroll=16),
        out_shape=jax.ShapeDtypeStruct((tokens, LANES), jnp.float32),
        in_specs=[
            pl.BlockSpec(memory_space=pltpu.SMEM),
            pl.BlockSpec(memory_space=pltpu.VMEM),
            pl.BlockSpec(memory_space=pltpu.VMEM),
        ],
        out_specs=pl.BlockSpec(memory_space=pltpu.VMEM),
        scratch_shapes=[pltpu.VMEM((tokens, LANES), jnp.float32)],
        compiler_params=pltpu.CompilerParams(vmem_limit_bytes=24 * 1024 * 1024),
        cost_estimate=pl.CostEstimate(
            flops=4 * tokens * width,
            bytes_accessed=4 * tokens * width,
            transcendentals=tokens * width,
        ),
    )(owner_order, logits, index)


def local(hidden_states, head_weight, pick_index, owner_order):
    shard_count = lax.axis_size("vocab")
    shard_start = lax.axis_index("vocab") * head_weight.shape[1]
    own_rows = hidden_states.shape[0]
    pick_count = pick_index.shape[1]
    logits = jnp.dot(
        lax.all_gather(hidden_states, "vocab", axis=0, tiled=True),
        head_weight,
        preferred_element_type=jnp.float32,
    )
    rows = picked_and_stats(logits, pick_index - shard_start, owner_order)
    rows = rows.reshape(shard_count, own_rows, LANES)
    received = lax.all_to_all(rows, "vocab", split_axis=0, concat_axis=0, tiled=True)
    maxima = received[:, :, LANES - 2]
    totals = received[:, :, LANES - 1]
    overall_max = jnp.max(maxima, axis=0)
    log_total = overall_max + jnp.log(
        jnp.sum(totals * jnp.exp(maxima - overall_max[None, :]), axis=0)
    )
    logprobs = jnp.sum(received[:, :, :pick_count], axis=0) - log_total[:, None]
    return (logprobs, log_total)


def solution(mesh):
    in_specs = (P(("group", "vocab"), None), P(None, "vocab"), P("group", None), P("group"))
    out_specs = (P(("group", "vocab"), None), P(("group", "vocab")))
    return jax.shard_map(local, mesh=mesh, in_specs=in_specs, out_specs=out_specs, check_vma=False)
```

```python
import functools

import jax
import jax.numpy as jnp
from jax import lax
from jax.experimental import pallas as pl
from jax.experimental.pallas import tpu as pltpu
from jax.sharding import PartitionSpec as P

LANES = 128
ROWS = 8
RING = 4
CORES = 2
TILE = 256
AXIS = "vocab"
STEPS = (0, 1, 3, 2)
CHUNKS = ((0,), (1, 2), (3,))


def index_of(x, z, core):
    return (x * RING + z) * CORES + core


def place_of(index):
    return index >> 3, (index >> 1) & 3, index & 1


def pairs(target):
    return [
        (index_of(x, z, c), index_of(*target(x, z, c)))
        for x in range(RING)
        for z in range(RING)
        for c in range(CORES)
    ]


def along(step, first_axis_core):
    return pairs(
        lambda x, z, c: ((x + step) % RING, z, c)
        if c == first_axis_core
        else (x, (z + step) % RING, c)
    )


def gathered_blocks(mine):
    x, z, c = place_of(mine)
    at = jnp.arange(RING * RING * CORES, dtype=jnp.int32)
    second, other, first = at >> 3, (at >> 2) & 1, at & 3
    second, first = second ^ (second >> 1), first ^ (first >> 1)
    core = c ^ other
    from_x = (x - jnp.where(core == 0, first, second)) & 3
    from_z = (z - jnp.where(core == 0, second, first)) & 3
    return index_of(from_x, from_z, core)


def rows_of(tokens, mine, block_rows):
    x, z, c = place_of(mine)
    shift = block_rows.bit_length() - 1
    block, row = tokens >> shift, tokens & (block_rows - 1)
    from_x, from_z, core = place_of(block)
    step_x = (x - from_x) & 3
    step_z = (z - from_z) & 3
    first = jnp.where(core == 0, step_x, step_z)
    second = jnp.where(core == 0, step_z, step_x)
    first, second = first ^ (first >> 1), second ^ (second >> 1)
    return ((second * CORES + (core ^ c)) * RING + first) * block_rows + row


def load(weight, after):
    depth, width = weight.shape

    def kernel(weight_ref, after_ref, out_ref, done):
        copy = pltpu.make_async_copy(weight_ref, out_ref, done)
        copy.start()
        copy.wait()

    return pl.pallas_call(
        kernel,
        out_shape=jax.ShapeDtypeStruct((depth, width), weight.dtype),
        in_specs=[pl.BlockSpec(memory_space=pltpu.HBM), pl.BlockSpec(memory_space=pl.ANY)],
        out_specs=pl.BlockSpec(memory_space=pltpu.VMEM),
        scratch_shapes=[pltpu.SemaphoreType.DMA],
        compiler_params=pltpu.CompilerParams(vmem_limit_bytes=32 * 1024 * 1024),
        cost_estimate=pl.CostEstimate(
            flops=256 * depth * width, bytes_accessed=4 * depth * width, transcendentals=0
        ),
    )(weight, after)


def chunk_kernel(*refs, pieces, ahead, start):
    block_ref, order_ref = refs[:2]
    x_refs = refs[2 : 2 + pieces]
    held_refs = refs[2 + pieces : 2 + pieces + ahead]
    refs = refs[2 + pieces + ahead :]
    weight_ref, index_ref, out_ref, x_all, index_here, even, odd, top_ref, sum_ref, found_ref, held = refs
    width = weight_ref.shape[1]
    count = x_all.shape[0]
    block_rows = index_ref.shape[0] // block_ref.shape[0]
    at = 0
    for x_ref in x_refs:
        x_all[at : at + x_ref.shape[0], :] = x_ref[...]
        at += x_ref.shape[0]
    for b in range(count // block_rows):
        rows = pl.ds(pl.multiple_of(block_ref[start // block_rows + b] * block_rows, block_rows), block_rows)
        index_here[b * block_rows : (b + 1) * block_rows, :] = index_ref[rows, :]

    def fold(logits, tile, columns):
        for b in range(count // ROWS):
            rows = slice(b * ROWS, (b + 1) * ROWS)
            wanted = index_here[rows, :]
            wanted_tile = lax.shift_right_arithmetic(wanted, 7)
            wanted_lane = lax.bitwise_and(wanted, LANES - 1)
            parts = [logits[rows, j * LANES : (j + 1) * LANES] for j in range(columns)]
            top = functools.reduce(jnp.maximum, parts)
            if tile:
                before = top_ref[rows, :]
                top = jnp.maximum(before, top)
            total = functools.reduce(jnp.add, [jnp.exp(p - top) for p in parts])
            if tile:
                total = total + sum_ref[rows, :] * jnp.exp(before - top)
                found = found_ref[rows, :]
            else:
                found = jnp.zeros((ROWS, LANES), jnp.float32)
            for j, part in enumerate(parts):
                seen = jnp.take_along_axis(part, wanted_lane, axis=1, mode="promise_in_bounds")
                found = jnp.where(wanted_tile == tile + j, seen, found)
            top_ref[rows, :] = top
            sum_ref[rows, :] = total
            found_ref[rows, :] = found

    waiting = None
    for t, left in enumerate(range(0, width, TILE)):
        right = min(left + TILE, width)
        logits = (even, odd)[t % 2]
        logits[:, : right - left] = jnp.dot(
            x_all[...], weight_ref[:, left:right], preferred_element_type=jnp.float32
        )
        if waiting is not None:
            fold(*waiting)
        waiting = (logits, left // LANES, (right - left) // LANES)
    fold(*waiting)
    lane = lax.broadcasted_iota(jnp.int32, (ROWS, LANES), 1)
    last = held is not None
    for b in range(count // ROWS):
        rows = slice(b * ROWS, (b + 1) * ROWS)
        tops = top_ref[rows, :]
        top = jnp.max(tops, axis=1, keepdims=True)
        total = jnp.sum(sum_ref[rows, :] * jnp.exp(tops - top), axis=1, keepdims=True)
        found = jnp.where(lane == LANES - 2, top, found_ref[rows, :])
        found = jnp.where(lane == LANES - 1, total, found)
        if last:
            held[start + b * ROWS : start + (b + 1) * ROWS, :] = found
        else:
            out_ref[rows, :] = found
    if last:
        at = 0
        for held_ref in held_refs:
            held[at : at + held_ref.shape[0], :] = held_ref[...]
            at += held_ref.shape[0]
        unroll = 16

        def move(b, _):
            for i in range(unroll):
                r = b * unroll + i
                out_ref[pl.ds(r, 1), :] = held[pl.ds(order_ref[r], 1), :]
            return 0

        lax.fori_loop(0, out_ref.shape[0] // unroll, move, 0)


def chunk(blocks, order, xs, held, weight, index, start, last):
    count = sum(x.shape[0] for x in xs)
    depth, width = weight.shape
    tokens = index.shape[0]
    scalar = pl.BlockSpec(memory_space=pltpu.SMEM)
    vector = pl.BlockSpec(memory_space=pltpu.VMEM)
    rows = pltpu.VMEM((count, LANES), jnp.float32)

    def kernel(*refs):
        refs = list(refs) + ([] if last else [None])
        chunk_kernel(*refs, pieces=len(xs), ahead=len(held), start=start)

    return pl.pallas_call(
        kernel,
        out_shape=jax.ShapeDtypeStruct((tokens if last else count, LANES), jnp.float32),
        in_specs=[scalar, scalar] + [vector] * (len(xs) + len(held) + 2),
        out_specs=vector,
        scratch_shapes=[
            pltpu.VMEM((count, depth), jnp.bfloat16),
            pltpu.VMEM((count, LANES), jnp.int32),
            pltpu.VMEM((count, TILE), jnp.float32),
            pltpu.VMEM((count, TILE), jnp.float32),
            rows,
            rows,
            rows,
        ]
        + ([pltpu.VMEM((tokens, LANES), jnp.float32)] if last else []),
        compiler_params=pltpu.CompilerParams(vmem_limit_bytes=16 * 1024 * 1024),
        cost_estimate=pl.CostEstimate(
            flops=2 * count * depth * width,
            bytes_accessed=2 * depth * width,
            transcendentals=count * width,
        ),
    )(blocks, order, *xs, *held, weight, index)


def local(hidden_states, head_weight, pick_index, owner_order):
    shard_count = lax.axis_size(AXIS)
    mine = lax.axis_index(AXIS)
    own_rows = hidden_states.shape[0]
    pick_count = pick_index.shape[1]
    blocks = gathered_blocks(mine)
    order = rows_of(owner_order, mine, own_rows)
    index = jnp.pad(
        pick_index - mine * head_weight.shape[1],
        ((0, 0), (0, LANES - pick_count)),
        constant_values=-1,
    )
    swap = pairs(lambda x, z, c: (x, z, 1 - c))
    arrived = [lax.ppermute(hidden_states, AXIS, along(k, 0)) for k in STEPS[1:]]
    line = jnp.concatenate([hidden_states] + arrived)
    plane = [line] + [lax.ppermute(line, AXIS, along(k, 1)) for k in STEPS[1:]]
    both = [(here, lax.ppermute(here, AXIS, swap)) for here in plane]
    weight = load(head_weight, line)
    held = []
    for n, members in enumerate(CHUNKS):
        xs = [x for j in members for x in both[j]]
        start = members[0] * 2 * line.shape[0]
        last = n == len(CHUNKS) - 1
        out = chunk(blocks, order, xs, held if last else [], weight, index, start, last)
        held.append(out)
    rows = held[-1].reshape(shard_count, own_rows, LANES)
    received = lax.all_to_all(rows, AXIS, split_axis=0, concat_axis=0, tiled=True)
    maxima = received[:, :, LANES - 2]
    totals = received[:, :, LANES - 1]
    overall_max = jnp.max(maxima, axis=0)
    log_total = overall_max + jnp.log(
        jnp.sum(totals * jnp.exp(maxima - overall_max[None, :]), axis=0)
    )
    logprobs = jnp.sum(received[:, :, :pick_count], axis=0) - log_total[:, None]
    return (logprobs, log_total)


def solution(mesh):
    in_specs = (P(("group", "vocab"), None), P(None, "vocab"), P("group", None), P("group"))
    out_specs = (P(("group", "vocab"), None), P(("group", "vocab")))
    return jax.shard_map(local, mesh=mesh, in_specs=in_specs, out_specs=out_specs, check_vma=False)
```

```python
import functools

import jax
import jax.numpy as jnp
from jax import lax
from jax.experimental import pallas as pl
from jax.experimental.pallas import tpu as pltpu
from jax.sharding import PartitionSpec as P

LANES = 128
ROWS = 8
RING = 4
CORES = 2
TILE = 256
AXIS = "vocab"
STEPS = (0, 1, 3, 2)
CHUNKS = (((0, 0), (0, 1)), ((1, 0), (2, 0)), ((1, 1), (2, 1)), ((3, 0), (3, 1)))
AHEAD = 3


def index_of(x, z, core):
    return (x * RING + z) * CORES + core


def place_of(index):
    return index >> 3, (index >> 1) & 3, index & 1


def pairs(target):
    return [
        (index_of(x, z, c), index_of(*target(x, z, c)))
        for x in range(RING)
        for z in range(RING)
        for c in range(CORES)
    ]


def along(step, first_axis_core):
    return pairs(
        lambda x, z, c: ((x + step) % RING, z, c)
        if c == first_axis_core
        else (x, (z + step) % RING, c)
    )


def gathered_blocks(mine):
    x, z, c = place_of(mine)
    at = jnp.arange(RING * RING * CORES, dtype=jnp.int32)
    second, other, first = at >> 3, (at >> 2) & 1, at & 3
    second, first = second ^ (second >> 1), first ^ (first >> 1)
    core = c ^ other
    from_x = (x - jnp.where(core == 0, first, second)) & 3
    from_z = (z - jnp.where(core == 0, second, first)) & 3
    return index_of(from_x, from_z, core)


def rows_of(tokens, mine, block_rows):
    x, z, c = place_of(mine)
    shift = block_rows.bit_length() - 1
    block, row = tokens >> shift, tokens & (block_rows - 1)
    from_x, from_z, core = place_of(block)
    step_x, step_z = (x - from_x) & 3, (z - from_z) & 3
    first = jnp.where(core == 0, step_x, step_z)
    second = jnp.where(core == 0, step_z, step_x)
    first, second, other = first ^ (first >> 1), second ^ (second >> 1), core ^ c
    piece = jnp.zeros_like(second)
    for n, (j, h) in enumerate(m for members in CHUNKS for m in members):
        piece = jnp.where((second == j) & (other == h), n, piece)
    return (piece * RING + first) * block_rows + row


def chunk_kernel(*refs, pieces, blocks, ahead, loads, last):
    refs = list(refs)

    def take(n):
        taken, refs[:n] = refs[:n], []
        return taken

    block_ref, order_ref = take(2)
    x_refs, held_refs = take(pieces), take(ahead)
    weight_ref, index_ref, out_ref = take(3)
    if loads:
        source_ref = weight_ref
        (weight_ref,) = take(1)
    x_all, index_here, even, odd, top_ref, sum_ref, found_ref = take(7)
    count = x_all.shape[0]
    width = weight_ref.shape[1]
    edges = [(left, min(left + TILE, width)) for left in range(0, width, TILE)]
    copies = []
    if loads:
        (done,) = take(1)
        copies = [
            pltpu.make_async_copy(source_ref.at[:, l:r], weight_ref.at[:, l:r], done.at[t])
            for t, (l, r) in enumerate(edges)
        ]
        for copy in copies[:AHEAD]:
            copy.start()
    at = 0
    for x_ref in x_refs:
        x_all[at : at + x_ref.shape[0], :] = x_ref[...]
        at += x_ref.shape[0]
    block_rows = index_ref.shape[0] // block_ref.shape[0]
    for b, block in enumerate(blocks):
        rows = pl.ds(pl.multiple_of(block_ref[block] * block_rows, block_rows), block_rows)
        index_here[b * block_rows : (b + 1) * block_rows, :] = index_ref[rows, :]

    def fold(logits, tile, columns):
        for b in range(count // ROWS):
            rows = slice(b * ROWS, (b + 1) * ROWS)
            wanted = index_here[rows, :]
            wanted_tile = lax.shift_right_arithmetic(wanted, 7)
            wanted_lane = lax.bitwise_and(wanted, LANES - 1)
            parts = [logits[rows, j * LANES : (j + 1) * LANES] for j in range(columns)]
            top = functools.reduce(jnp.maximum, parts)
            if tile:
                before = top_ref[rows, :]
                top = jnp.maximum(before, top)
            total = functools.reduce(jnp.add, [jnp.exp(p - top) for p in parts])
            if tile:
                total = total + sum_ref[rows, :] * jnp.exp(before - top)
                found = found_ref[rows, :]
            else:
                found = jnp.zeros((ROWS, LANES), jnp.float32)
            for j, part in enumerate(parts):
                seen = jnp.take_along_axis(part, wanted_lane, axis=1, mode="promise_in_bounds")
                found = jnp.where(wanted_tile == tile + j, seen, found)
            top_ref[rows, :] = top
            sum_ref[rows, :] = total
            found_ref[rows, :] = found

    waiting = None
    for t, (left, right) in enumerate(edges):
        if copies:
            copies[t].wait()
            if t + AHEAD < len(copies):
                copies[t + AHEAD].start()
        logits = (even, odd)[t % 2]
        logits[:, : right - left] = jnp.dot(
            x_all[...], weight_ref[:, left:right], preferred_element_type=jnp.float32
        )
        if waiting is not None:
            fold(*waiting)
        waiting = (logits, left // LANES, (right - left) // LANES)
    fold(*waiting)
    lane = lax.broadcasted_iota(jnp.int32, (ROWS, LANES), 1)
    if last:
        (held,) = take(1)
        at = 0
        for held_ref in held_refs:
            held[at : at + held_ref.shape[0], :] = held_ref[...]
            at += held_ref.shape[0]
    for b in range(count // ROWS):
        rows = slice(b * ROWS, (b + 1) * ROWS)
        tops = top_ref[rows, :]
        top = jnp.max(tops, axis=1, keepdims=True)
        total = jnp.sum(sum_ref[rows, :] * jnp.exp(tops - top), axis=1, keepdims=True)
        found = jnp.where(lane == LANES - 2, top, found_ref[rows, :])
        found = jnp.where(lane == LANES - 1, total, found)
        if last:
            held[at + b * ROWS : at + (b + 1) * ROWS, :] = found
        else:
            out_ref[rows, :] = found
    if last:
        unroll = 16

        def move(b, _):
            for i in range(unroll):
                r = b * unroll + i
                out_ref[pl.ds(r, 1), :] = held[pl.ds(order_ref[r], 1), :]
            return 0

        lax.fori_loop(0, out_ref.shape[0] // unroll, move, 0)


def chunk(blocks, order, xs, members, held, weight, index, loads=False, last=False):
    count = sum(x.shape[0] for x in xs)
    depth, width = weight.shape
    tokens = index.shape[0]
    scalar = pl.BlockSpec(memory_space=pltpu.SMEM)
    vector = pl.BlockSpec(memory_space=pltpu.VMEM)
    rows = pltpu.VMEM((count, LANES), jnp.float32)
    out_shape = [jax.ShapeDtypeStruct((tokens if last else count, LANES), jnp.float32)]
    scratch = [
        pltpu.VMEM((count, depth), jnp.bfloat16),
        pltpu.VMEM((count, LANES), jnp.int32),
        pltpu.VMEM((count, TILE), jnp.float32),
        pltpu.VMEM((count, TILE), jnp.float32),
        rows,
        rows,
        rows,
    ]
    if loads:
        out_shape.append(jax.ShapeDtypeStruct((depth, width), weight.dtype))
        scratch.append(pltpu.SemaphoreType.DMA((pl.cdiv(width, TILE),)))
    if last:
        scratch.append(pltpu.VMEM((tokens, LANES), jnp.float32))
    out = pl.pallas_call(
        functools.partial(
            chunk_kernel,
            pieces=len(xs),
            blocks=members,
            ahead=len(held),
            loads=loads,
            last=last,
        ),
        out_shape=out_shape,
        in_specs=[scalar, scalar]
        + [vector] * (len(xs) + len(held))
        + [pl.BlockSpec(memory_space=pltpu.HBM) if loads else vector, vector],
        out_specs=[vector] * len(out_shape),
        scratch_shapes=scratch,
        compiler_params=pltpu.CompilerParams(
            vmem_limit_bytes=(26 if loads else 16) * 1024 * 1024
        ),
        cost_estimate=pl.CostEstimate(
            flops=2 * count * depth * width,
            bytes_accessed=2 * depth * width,
            transcendentals=count * width,
        ),
    )(blocks, order, *xs, *held, weight, index)
    return out if loads else out[0]


def combine_kernel(rows_ref, logprobs_ref, log_total_ref):
    rows = rows_ref[...]
    shards, own, _ = rows.shape
    shifted = pltpu.roll(rows.reshape(shards * own, LANES), 1, 1).reshape(rows.shape)
    top = jnp.max(shifted, axis=0)
    total = jnp.sum(rows * jnp.exp(shifted - top[None]), axis=0)
    lane = lax.broadcasted_iota(jnp.int32, (own, LANES), 1)
    log_total = jnp.where(lane == LANES - 1, top + jnp.log(total), 0.0)
    log_total = jnp.sum(log_total, axis=1, keepdims=True)
    picks = logprobs_ref.shape[1]
    logprobs_ref[...] = jnp.sum(rows, axis=0)[:, :picks] - log_total
    row = lax.broadcasted_iota(jnp.int32, (own, LANES), 0)
    line = jnp.sum(jnp.where(row == lane, log_total, 0.0), axis=0, keepdims=True)
    log_total_ref[...] = line[:, :own]


def combine(rows, picks):
    own = rows.shape[1]
    vector = pl.BlockSpec(memory_space=pltpu.VMEM)
    logprobs, log_total = pl.pallas_call(
        combine_kernel,
        out_shape=[
            jax.ShapeDtypeStruct((own, picks), jnp.float32),
            jax.ShapeDtypeStruct((1, own), jnp.float32),
        ],
        in_specs=[vector],
        out_specs=[vector, vector],
        compiler_params=pltpu.CompilerParams(vmem_limit_bytes=4 * 1024 * 1024),
    )(rows)
    return logprobs, log_total.reshape(own)


def local(hidden_states, head_weight, pick_index, owner_order):
    shard_count = lax.axis_size(AXIS)
    mine = lax.axis_index(AXIS)
    own_rows = hidden_states.shape[0]
    pick_count = pick_index.shape[1]
    blocks = gathered_blocks(mine)
    order = rows_of(owner_order, mine, own_rows)
    index = jnp.pad(
        pick_index - mine * head_weight.shape[1],
        ((0, 0), (0, LANES - pick_count)),
        constant_values=-1,
    )
    swap = pairs(lambda x, z, c: (x, z, 1 - c))
    arrived = [lax.ppermute(hidden_states, AXIS, along(k, 0)) for k in STEPS[1:]]
    *arrived, blocks, order, index = lax.optimization_barrier((*arrived, blocks, order, index))
    line = jnp.concatenate([hidden_states] + arrived)
    plane = [line] + [lax.ppermute(line, AXIS, along(k, 1)) for k in STEPS[1:]]
    pieces = {(0, 0): line, (0, 1): lax.ppermute(line, AXIS, swap)}

    def run(n, held, weight, **kw):
        members = CHUNKS[n]
        xs = [pieces[m] for m in members]
        at = [(j * CORES + h) * RING + i for j, h in members for i in range(RING)]
        return chunk(blocks, order, xs, at, held, weight, index, **kw)

    first, weight = run(0, [], head_weight, loads=True)
    *plane[1:], first = lax.optimization_barrier((*plane[1:], first))
    for j in range(1, RING):
        pieces[j, 0], pieces[j, 1] = plane[j], lax.ppermute(plane[j], AXIS, swap)
    held = [first]
    for n in range(1, len(CHUNKS)):
        last = n == len(CHUNKS) - 1
        held.append(run(n, held if last else [], weight, last=last))
    rows = held[-1].reshape(shard_count, own_rows, LANES)
    received = lax.all_to_all(rows, AXIS, split_axis=0, concat_axis=0, tiled=True)
    return combine(received, pick_count)


def solution(mesh):
    in_specs = (P(("group", "vocab"), None), P(None, "vocab"), P("group", None), P("group"))
    out_specs = (P(("group", "vocab"), None), P(("group", "vocab")))
    return jax.shard_map(local, mesh=mesh, in_specs=in_specs, out_specs=out_specs, check_vma=False)
```

```python
import functools

import jax
import jax.numpy as jnp
import numpy as np
from jax import lax
from jax.experimental import pallas as pl
from jax.experimental.pallas import tpu as pltpu
from jax.sharding import PartitionSpec as P


LANES = 128
ROWS = 8
RING = 4
CORES = 2
TILE = 512
AXIS = "vocab"
STEPS = (0, 1, 3, 2)
AHEAD = 3
SETTLE_FLOPS = 1 << 34


def index_of(x, z, core):
    return (x * RING + z) * CORES + core


def place_of(index):
    return index >> 3, (index >> 1) & 3, index & 1


def pairs(target):
    return [
        (index_of(x, z, c), index_of(*target(x, z, c)))
        for x in range(RING)
        for z in range(RING)
        for c in range(CORES)
    ]


def along(step, first_axis_core):
    return pairs(
        lambda x, z, c: ((x + step) % RING, z, c)
        if c == first_axis_core
        else (x, (z + step) % RING, c)
    )


def settle(blocks):
    def kernel(blocks_ref, out_ref):
        out_ref[...] = blocks_ref[...]

    vector = pl.BlockSpec(memory_space=pltpu.VMEM)
    return pl.pallas_call(
        kernel,
        out_shape=jax.ShapeDtypeStruct(blocks.shape, blocks.dtype),
        in_specs=[vector],
        out_specs=vector,
        compiler_params=pltpu.CompilerParams(vmem_limit_bytes=1024 * 1024),
        cost_estimate=pl.CostEstimate(
            flops=SETTLE_FLOPS, bytes_accessed=1024, transcendentals=0
        ),
    )(blocks)


def gathered_blocks(mine, arrivals):
    x, z, c = place_of(mine)
    at = np.array([(STEPS[second], STEPS[first], other) for second, first, other in arrivals])
    second, first, other = (jnp.asarray(v, jnp.int32) for v in at.T)
    core = c ^ other
    from_x = (x - jnp.where(core == 0, first, second)) & 3
    from_z = (z - jnp.where(core == 0, second, first)) & 3
    return index_of(from_x, from_z, core)


def chunk_kernel(*refs, pieces, blocks, ahead, loads, last):
    refs = list(refs)

    def take(n):
        taken, refs[:n] = refs[:n], []
        return taken

    (block_ref,) = take(1)
    if last:
        (order_ref,) = take(1)
    x_refs, held_refs = take(pieces), take(ahead)
    weight_ref, index_ref, out_ref = take(3)
    if loads:
        source_ref, picks_ref = weight_ref, index_ref
        weight_ref, index_ref = take(2)
    x_all, index_here, even, odd, top_ref, sum_ref, found_ref = take(7)
    count = x_all.shape[0]
    width = weight_ref.shape[1]
    edges = [(left, min(left + TILE, width)) for left in range(0, width, TILE)]
    copies = []
    if loads:
        (done,) = take(1)
        copies = [
            pltpu.make_async_copy(source_ref.at[:, l:r], weight_ref.at[:, l:r], done.at[t])
            for t, (l, r) in enumerate(edges)
        ]
        for copy in copies[:AHEAD]:
            copy.start()
    if loads:
        picks, tokens = picks_ref.shape
        for left in range(0, tokens, LANES):
            some = picks_ref[:, left : left + LANES]
            more = jnp.full((LANES - picks, LANES), -1, jnp.int32)
            index_ref[left : left + LANES, :] = jnp.concatenate([some, more], axis=0).T
    at = 0
    for x_ref in x_refs:
        x_all[at : at + x_ref.shape[0], :] = x_ref[...]
        at += x_ref.shape[0]
    block_rows = index_ref.shape[0] // block_ref.shape[0]

    def rows_of(block):
        return pl.ds(pl.multiple_of(block_ref[block] * block_rows, block_rows), block_rows)

    start = lax.axis_index(AXIS) * width
    for b, block in enumerate(blocks):
        index_here[b * block_rows : (b + 1) * block_rows, :] = index_ref[rows_of(block), :] - start

    def fold(logits, tile, columns):
        for b in range(count // ROWS):
            rows = slice(b * ROWS, (b + 1) * ROWS)
            wanted = index_here[rows, :]
            wanted_tile = lax.shift_right_arithmetic(wanted, 7)
            wanted_lane = lax.bitwise_and(wanted, LANES - 1)
            parts = [logits[rows, j * LANES : (j + 1) * LANES] for j in range(columns)]
            top = functools.reduce(jnp.maximum, parts)
            if tile:
                before = top_ref[rows, :]
                top = jnp.maximum(before, top)
            total = functools.reduce(jnp.add, [jnp.exp(p - top) for p in parts])
            if tile:
                total = total + sum_ref[rows, :] * jnp.exp(before - top)
                found = found_ref[rows, :]
            else:
                found = jnp.zeros((ROWS, LANES), jnp.float32)
            for j, part in enumerate(parts):
                seen = jnp.take_along_axis(part, wanted_lane, axis=1, mode="promise_in_bounds")
                found = jnp.where(wanted_tile == tile + j, seen, found)
            top_ref[rows, :] = top
            sum_ref[rows, :] = total
            found_ref[rows, :] = found

    waiting = None
    for t, (left, right) in enumerate(edges):
        if copies:
            copies[t].wait()
            if t + AHEAD < len(copies):
                copies[t + AHEAD].start()
        logits = (even, odd)[t % 2]
        logits[:, : right - left] = jnp.dot(
            x_all[...], weight_ref[:, left:right], preferred_element_type=jnp.float32
        )
        if waiting is not None:
            fold(*waiting)
        waiting = (logits, left // LANES, (right - left) // LANES)
    fold(*waiting)
    lane = lax.broadcasted_iota(jnp.int32, (ROWS, LANES), 1)
    rest = out_ref
    if last:
        held, rest = take(2)
    for b in range(count // ROWS):
        rows = slice(b * ROWS, (b + 1) * ROWS)
        tops = top_ref[rows, :]
        top = jnp.max(tops, axis=1, keepdims=True)
        total = jnp.sum(sum_ref[rows, :] * jnp.exp(tops - top), axis=1, keepdims=True)
        found = jnp.where(lane == LANES - 2, top, found_ref[rows, :])
        rest[rows, :] = jnp.where(lane == LANES - 1, total, found)
    if last:
        block = 0
        for held_ref in [*held_refs, rest]:
            for at in range(0, held_ref.shape[0], block_rows):
                held[rows_of(block), :] = held_ref[at : at + block_rows, :]
                block += 1
    if last:
        unroll = 16

        def move(b, _):
            for i in range(unroll):
                r = b * unroll + i
                out_ref[pl.ds(r, 1), :] = held[pl.ds(order_ref[r], 1), :]
            return 0

        lax.fori_loop(0, out_ref.shape[0] // unroll, move, 0)


def chunk(blocks, xs, members, held, weight, index, order=None, loads=False):
    last = order is not None
    count = sum(x.shape[0] for x in xs)
    depth, width = weight.shape
    tokens = index.shape[1 if loads else 0]
    scalar = pl.BlockSpec(memory_space=pltpu.SMEM)
    vector = pl.BlockSpec(memory_space=pltpu.VMEM)
    rows = pltpu.VMEM((count, LANES), jnp.float32)
    out_shape = [jax.ShapeDtypeStruct((tokens if last else count, LANES), jnp.float32)]
    scratch = [
        pltpu.VMEM((count, depth), jnp.bfloat16),
        pltpu.VMEM((count, LANES), jnp.int32),
        pltpu.VMEM((count, TILE), jnp.float32),
        pltpu.VMEM((count, TILE), jnp.float32),
        rows,
        rows,
        rows,
    ]
    if loads:
        out_shape.append(jax.ShapeDtypeStruct((depth, width), weight.dtype))
        out_shape.append(jax.ShapeDtypeStruct((tokens, LANES), jnp.int32))
        scratch.append(pltpu.SemaphoreType.DMA((pl.cdiv(width, TILE),)))
    if last:
        scratch += [pltpu.VMEM((tokens, LANES), jnp.float32), rows]
    out = pl.pallas_call(
        functools.partial(
            chunk_kernel,
            pieces=len(xs),
            blocks=members,
            ahead=len(held),
            loads=loads,
            last=last,
        ),
        out_shape=out_shape,
        in_specs=[scalar] * (2 if last else 1)
        + [vector] * (len(xs) + len(held))
        + [pl.BlockSpec(memory_space=pltpu.HBM) if loads else vector, vector],
        out_specs=[vector] * len(out_shape),
        scratch_shapes=scratch,
        compiler_params=pltpu.CompilerParams(
            vmem_limit_bytes=(22 if loads else 16) * 1024 * 1024
        ),
        cost_estimate=pl.CostEstimate(
            flops=2 * count * depth * width,
            bytes_accessed=2 * depth * width,
            transcendentals=count * width,
        ),
    )(blocks, *([order] if last else []), *xs, *held, weight, index)
    return out if loads else out[0]


def combine_kernel(rows_ref, logprobs_ref, log_total_ref):
    rows = rows_ref[...]
    shards, own, _ = rows.shape
    shifted = pltpu.roll(rows.reshape(shards * own, LANES), 1, 1).reshape(rows.shape)
    top = jnp.max(shifted, axis=0)
    total = jnp.sum(rows * jnp.exp(shifted - top[None]), axis=0)
    lane = lax.broadcasted_iota(jnp.int32, (own, LANES), 1)
    log_total = jnp.where(lane == LANES - 1, top + jnp.log(total), 0.0)
    log_total = jnp.sum(log_total, axis=1, keepdims=True)
    picks = logprobs_ref.shape[1]
    logprobs_ref[...] = jnp.sum(rows, axis=0)[:, :picks] - log_total
    row = lax.broadcasted_iota(jnp.int32, (own, LANES), 0)
    line = jnp.sum(jnp.where(row == lane, log_total, 0.0), axis=0, keepdims=True)
    log_total_ref[...] = line[:, :own]


def combine(rows, picks):
    own = rows.shape[1]
    vector = pl.BlockSpec(memory_space=pltpu.VMEM)
    logprobs, log_total = pl.pallas_call(
        combine_kernel,
        out_shape=[
            jax.ShapeDtypeStruct((own, picks), jnp.float32),
            jax.ShapeDtypeStruct((1, own), jnp.float32),
        ],
        in_specs=[vector],
        out_specs=[vector, vector],
        compiler_params=pltpu.CompilerParams(vmem_limit_bytes=4 * 1024 * 1024),
    )(rows)
    return logprobs, log_total.reshape(own)


def shifts(value, phase):
    received = []
    for k in STEPS[1:]:
        received.append(lax.ppermute(value, AXIS, along(k, phase)))
    return received


def program(hidden_states, head_weight, pick_index, owner_order):
    shard_count = lax.axis_size(AXIS)
    mine = lax.axis_index(AXIS)
    own_rows = hidden_states.shape[0]
    pick_count = pick_index.shape[1]
    swap = pairs(lambda x, z, c: (x, z, 1 - c))

    def swapped(value):
        return lax.ppermute(value, AXIS, swap)

    own = hidden_states
    line = jnp.concatenate(shifts(own, 0))
    cross = jnp.concatenate(shifts(own, 1))
    rest = shifts(line, 1)
    early = {"own": own, "line": line, "cross": cross}
    steps = range(1, RING)
    members = [(0, 0)] + [(0, i) for i in steps] + [(j, 0) for j in steps]
    late = [(j, i) for j in steps for i in steps]
    arrivals = [
        (j, i, other) for group in (members, late) for other in (0, 1) for j, i in group
    ]
    blocks = settle(gathered_blocks(mine, arrivals))
    at = list(range(shard_count))
    cut = 2 * len(members), 2 * len(members) + len(late)
    others = [swapped(v) for v in early.values()]
    xs = [*early.values(), *others]
    first, weight, index = chunk(
        blocks, xs, at[: cut[0]], [], head_weight, pick_index.T, loads=True
    )
    *rest, first = lax.optimization_barrier((*rest, first))
    second = chunk(blocks, rest, at[cut[0] : cut[1]], [], weight, index)
    others = [swapped(v) for v in rest]
    held = [first, second]
    rows = chunk(blocks, others, at[cut[1] :], held, weight, index, order=owner_order)
    rows = rows.reshape(shard_count, own_rows, LANES)
    received = lax.all_to_all(rows, AXIS, split_axis=0, concat_axis=0, tiled=True)
    return combine(received, pick_count)


def solution(mesh):
    in_specs = (P(("group", "vocab"), None), P(None, "vocab"), P("group", None), P("group"))
    out_specs = (P(("group", "vocab"), None), P(("group", "vocab")))
    return jax.shard_map(
        program, mesh=mesh, in_specs=in_specs, out_specs=out_specs, check_vma=False
    )
```

```python
import functools

import jax
import jax.numpy as jnp
from jax import lax
from jax.experimental import pallas as pl
from jax.experimental.pallas import tpu as pltpu
from jax.sharding import PartitionSpec as P


LANES = 128
ROWS = 8
RING = 4
CORES = 2
TILE = 512
AXIS = "vocab"
STEPS = (0, 1, 3, 2)
COVER_FLOPS = 1 << 35
EARLY = 2 * RING - 1
LATE = (RING - 1) ** 2


def index_of(x, z, core):
    return (x * RING + z) * CORES + core


def place_of(index):
    return index >> 3, (index >> 1) & 3, index & 1


def pairs(target):
    return [
        (index_of(x, z, c), index_of(*target(x, z, c)))
        for x in range(RING)
        for z in range(RING)
        for c in range(CORES)
    ]


def along(step, first_axis_core):
    return pairs(
        lambda x, z, c: ((x + step) % RING, z, c)
        if c == first_axis_core
        else (x, (z + step) % RING, c)
    )


def table_kernel(out_ref):
    x, z, c = place_of(lax.axis_index(AXIS))
    at = lax.broadcasted_iota(jnp.int32, out_ref.shape, 1)
    late = at - 2 * EARLY
    one = jnp.ones_like(at)
    other = jnp.where(at >= EARLY, one, 0) - jnp.where(late >= 0, one, 0) + jnp.where(late >= LATE, one, 0)
    soon = at - EARLY * other
    late = late - LATE * other
    turn = jnp.where(late >= RING - 1, one, 0) + jnp.where(late >= 2 * (RING - 1), one, 0)
    second = jnp.where(at < 2 * EARLY, jnp.maximum(soon - (RING - 1), 0), 1 + turn)
    first = jnp.where(soon >= RING, 0, soon)
    first = jnp.where(at < 2 * EARLY, first, 1 + late - (RING - 1) * turn)
    first, second = first ^ (first >> 1), second ^ (second >> 1)
    core = c ^ other
    from_x = (x - jnp.where(core == 0, first, second)) & 3
    from_z = (z - jnp.where(core == 0, second, first)) & 3
    out_ref[...] = index_of(from_x, from_z, core)


def table():
    return pl.pallas_call(
        table_kernel,
        out_shape=jax.ShapeDtypeStruct((1, LANES), jnp.int32),
        out_specs=pl.BlockSpec(memory_space=pltpu.VMEM),
        compiler_params=pltpu.CompilerParams(vmem_limit_bytes=1024 * 1024),
        cost_estimate=pl.CostEstimate(flops=COVER_FLOPS, bytes_accessed=1024, transcendentals=0),
    )()


def chunk_kernel(*refs, pieces, blocks, ahead, first, last):
    refs = list(refs)

    def take(n):
        taken, refs[:n] = refs[:n], []
        return taken

    (block_ref,) = take(1)
    if last:
        (order_ref,) = take(1)
    x_refs, held_refs = take(pieces), take(ahead)
    weight_ref, index_ref, out_ref = take(3)
    if first:
        picks_ref = index_ref
        (index_ref,) = take(1)
    x_all, index_here, even, odd, top_ref, sum_ref, found_ref = take(7)
    count = x_all.shape[0]
    width = weight_ref.shape[1]
    edges = [(left, min(left + TILE, width)) for left in range(0, width, TILE)]
    if first:
        picks, tokens = picks_ref.shape
        for left in range(0, tokens, LANES):
            some = picks_ref[:, left : left + LANES]
            more = jnp.full((LANES - picks, LANES), -1, jnp.int32)
            index_ref[left : left + LANES, :] = jnp.concatenate([some, more], axis=0).T
    at = 0
    for x_ref in x_refs:
        x_all[at : at + x_ref.shape[0], :] = x_ref[...]
        at += x_ref.shape[0]
    block_rows = index_ref.shape[0] // (RING * RING * CORES)

    def rows_of(block):
        return pl.ds(pl.multiple_of(block_ref[0, block] * block_rows, block_rows), block_rows)

    start = lax.axis_index(AXIS) * width
    for b, block in enumerate(blocks):
        index_here[b * block_rows : (b + 1) * block_rows, :] = index_ref[rows_of(block), :] - start

    def fold(logits, tile, columns):
        for b in range(count // ROWS):
            rows = slice(b * ROWS, (b + 1) * ROWS)
            wanted = index_here[rows, :]
            wanted_tile = lax.shift_right_arithmetic(wanted, 7)
            wanted_lane = lax.bitwise_and(wanted, LANES - 1)
            parts = [logits[rows, j * LANES : (j + 1) * LANES] for j in range(columns)]
            top = functools.reduce(jnp.maximum, parts)
            if tile:
                before = top_ref[rows, :]
                top = jnp.maximum(before, top)
            total = functools.reduce(jnp.add, [jnp.exp(p - top) for p in parts])
            if tile:
                total = total + sum_ref[rows, :] * jnp.exp(before - top)
                found = found_ref[rows, :]
            else:
                found = jnp.zeros((ROWS, LANES), jnp.float32)
            for j, part in enumerate(parts):
                seen = jnp.take_along_axis(part, wanted_lane, axis=1, mode="promise_in_bounds")
                found = jnp.where(wanted_tile == tile + j, seen, found)
            top_ref[rows, :] = top
            sum_ref[rows, :] = total
            found_ref[rows, :] = found

    waiting = None
    for t, (left, right) in enumerate(edges):
        logits = (even, odd)[t % 2]
        logits[:, : right - left] = jnp.dot(
            x_all[...], weight_ref[:, left:right], preferred_element_type=jnp.float32
        )
        if waiting is not None:
            fold(*waiting)
        waiting = (logits, left // LANES, (right - left) // LANES)
    fold(*waiting)
    lane = lax.broadcasted_iota(jnp.int32, (ROWS, LANES), 1)
    rest = out_ref
    if last:
        held, rest = take(2)
    for b in range(count // ROWS):
        rows = slice(b * ROWS, (b + 1) * ROWS)
        tops = top_ref[rows, :]
        top = jnp.max(tops, axis=1, keepdims=True)
        total = jnp.sum(sum_ref[rows, :] * jnp.exp(tops - top), axis=1, keepdims=True)
        found = jnp.where(lane == LANES - 2, top, found_ref[rows, :])
        rest[rows, :] = jnp.where(lane == LANES - 1, total, found)
    if last:
        block = 0
        for held_ref in [*held_refs, rest]:
            for at in range(0, held_ref.shape[0], block_rows):
                held[rows_of(block), :] = held_ref[at : at + block_rows, :]
                block += 1
    if last:
        unroll = 16

        def move(b, _):
            for i in range(unroll):
                r = b * unroll + i
                out_ref[pl.ds(r, 1), :] = held[pl.ds(order_ref[r], 1), :]
            return 0

        lax.fori_loop(0, out_ref.shape[0] // unroll, move, 0)


def chunk(blocks, xs, members, held, weight, index, order=None, first=False):
    last = order is not None
    count = sum(x.shape[0] for x in xs)
    depth, width = weight.shape
    tokens = index.shape[1 if first else 0]
    scalar = pl.BlockSpec(memory_space=pltpu.SMEM)
    vector = pl.BlockSpec(memory_space=pltpu.VMEM)
    rows = pltpu.VMEM((count, LANES), jnp.float32)
    out_shape = [jax.ShapeDtypeStruct((tokens if last else count, LANES), jnp.float32)]
    scratch = [
        pltpu.VMEM((count, depth), jnp.bfloat16),
        pltpu.VMEM((count, LANES), jnp.int32),
        pltpu.VMEM((count, TILE), jnp.float32),
        pltpu.VMEM((count, TILE), jnp.float32),
        rows,
        rows,
        rows,
    ]
    if first:
        out_shape.append(jax.ShapeDtypeStruct((tokens, LANES), jnp.int32))
    if last:
        scratch += [pltpu.VMEM((tokens, LANES), jnp.float32), rows]
    out = pl.pallas_call(
        functools.partial(
            chunk_kernel,
            pieces=len(xs),
            blocks=members,
            ahead=len(held),
            first=first,
            last=last,
        ),
        out_shape=out_shape,
        in_specs=[scalar] * (2 if last else 1)
        + [vector] * (len(xs) + len(held) + 2),
        out_specs=[vector] * len(out_shape),
        scratch_shapes=scratch,
        compiler_params=pltpu.CompilerParams(vmem_limit_bytes=12 * 1024 * 1024),
        cost_estimate=pl.CostEstimate(
            flops=2 * count * depth * width,
            bytes_accessed=2 * depth * width,
            transcendentals=count * width,
        ),
    )(blocks, *([order] if last else []), *xs, *held, weight, index)
    return out if first else out[0]


def combine_kernel(rows_ref, logprobs_ref, log_total_ref):
    rows = rows_ref[...]
    shards, own, _ = rows.shape
    shifted = pltpu.roll(rows.reshape(shards * own, LANES), 1, 1).reshape(rows.shape)
    top = jnp.max(shifted, axis=0)
    total = jnp.sum(rows * jnp.exp(shifted - top[None]), axis=0)
    lane = lax.broadcasted_iota(jnp.int32, (own, LANES), 1)
    log_total = jnp.where(lane == LANES - 1, top + jnp.log(total), 0.0)
    log_total = jnp.sum(log_total, axis=1, keepdims=True)
    picks = logprobs_ref.shape[1]
    logprobs_ref[...] = jnp.sum(rows, axis=0)[:, :picks] - log_total
    row = lax.broadcasted_iota(jnp.int32, (own, LANES), 0)
    line = jnp.sum(jnp.where(row == lane, log_total, 0.0), axis=0, keepdims=True)
    log_total_ref[...] = line[:, :own]


def combine(rows, picks):
    own = rows.shape[1]
    vector = pl.BlockSpec(memory_space=pltpu.VMEM)
    logprobs, log_total = pl.pallas_call(
        combine_kernel,
        out_shape=[
            jax.ShapeDtypeStruct((own, picks), jnp.float32),
            jax.ShapeDtypeStruct((1, own), jnp.float32),
        ],
        in_specs=[vector],
        out_specs=[vector, vector],
        compiler_params=pltpu.CompilerParams(vmem_limit_bytes=4 * 1024 * 1024),
    )(rows)
    return logprobs, log_total.reshape(own)


def shifts(value, phase):
    received = []
    for k in STEPS[1:]:
        received.append(lax.ppermute(value, AXIS, along(k, phase)))
    return received


def program(hidden_states, head_weight, pick_index, owner_order):
    shard_count = lax.axis_size(AXIS)
    own_rows = hidden_states.shape[0]
    pick_count = pick_index.shape[1]
    swap = pairs(lambda x, z, c: (x, z, 1 - c))

    def swapped(value):
        return lax.ppermute(value, AXIS, swap)

    blocks = table()
    own = hidden_states
    line = jnp.concatenate(shifts(own, 0))
    cross = jnp.concatenate(shifts(own, 1))
    rest = shifts(line, 1)
    early = {"own": own, "line": line, "cross": cross}
    at = list(range(shard_count))
    cut = 2 * EARLY, 2 * EARLY + LATE
    others = [swapped(v) for v in early.values()]
    xs = [*early.values(), *others]
    first, index = chunk(blocks, xs, at[: cut[0]], [], head_weight, pick_index.T, first=True)
    *rest, first = lax.optimization_barrier((*rest, first))
    second = chunk(blocks, rest, at[cut[0] : cut[1]], [], head_weight, index)
    others = [swapped(v) for v in rest]
    held = [first, second]
    rows = chunk(blocks, others, at[cut[1] :], held, head_weight, index, order=owner_order)
    rows = rows.reshape(shard_count, own_rows, LANES)
    received = lax.all_to_all(rows, AXIS, split_axis=0, concat_axis=0, tiled=True)
    return combine(received, pick_count)


def solution(mesh):
    in_specs = (P(("group", "vocab"), None), P(None, "vocab"), P("group", None), P("group"))
    out_specs = (P(("group", "vocab"), None), P(("group", "vocab")))
    return jax.shard_map(
        program, mesh=mesh, in_specs=in_specs, out_specs=out_specs, check_vma=False
    )
```

```python
import functools

import jax
import jax.numpy as jnp
from jax import lax
from jax.experimental import pallas as pl
from jax.experimental.pallas import tpu as pltpu
from jax.sharding import PartitionSpec as P


LANES = 128
ROWS = 8
RING = 4
CORES = 2
TILE = 512
AXIS = "vocab"
STEPS = (0, 1, 3, 2)
COVER_FLOPS = 1 << 35


def index_of(x, z, core):
    return (x * RING + z) * CORES + core


def place_of(index):
    return index >> 3, (index >> 1) & 3, index & 1


def pairs(target):
    return [
        (index_of(x, z, c), index_of(*target(x, z, c)))
        for x in range(RING)
        for z in range(RING)
        for c in range(CORES)
    ]


def along(step, first_axis_core):
    return pairs(
        lambda x, z, c: ((x + step) % RING, z, c)
        if c == first_axis_core
        else (x, (z + step) % RING, c)
    )


def arrivals():
    steps = range(1, RING)
    early = [(0, 0)] + [(0, i) for i in steps] + [(j, 0) for j in steps]
    late = [(j, i) for j in steps for i in steps]
    near = RING - 1 << 1
    return [
        [(*b, other) for other in range(CORES) for b in early],
        [(*b, 0) for b in late[:near]],
        [(*b, 0) for b in late[near:]] + [(*b, 1) for b in late],
    ]


def table_kernel(out_ref):
    x, z, c = place_of(lax.axis_index(AXIS))
    at = lax.broadcasted_iota(jnp.int32, out_ref.shape, 1)
    second = first = other = jnp.zeros_like(at)
    for n, (j, i, swapped) in enumerate(b for part in arrivals() for b in part):
        second = jnp.where(at == n, STEPS[j], second)
        first = jnp.where(at == n, STEPS[i], first)
        other = jnp.where(at == n, swapped, other)
    core = c ^ other
    from_x = (x - jnp.where(core == 0, first, second)) & 3
    from_z = (z - jnp.where(core == 0, second, first)) & 3
    out_ref[...] = index_of(from_x, from_z, core)


def table():
    return pl.pallas_call(
        table_kernel,
        out_shape=jax.ShapeDtypeStruct((1, LANES), jnp.int32),
        out_specs=pl.BlockSpec(memory_space=pltpu.VMEM),
        compiler_params=pltpu.CompilerParams(vmem_limit_bytes=1024 * 1024),
        cost_estimate=pl.CostEstimate(flops=COVER_FLOPS, bytes_accessed=1024, transcendentals=0),
    )()


def chunk_kernel(*refs, pieces, blocks, ahead, first, last):
    refs = list(refs)

    def take(n):
        taken, refs[:n] = refs[:n], []
        return taken

    (block_ref,) = take(1)
    if last:
        (order_ref,) = take(1)
    x_refs, held_refs = take(pieces), take(ahead)
    weight_ref, index_ref, out_ref = take(3)
    if first:
        picks_ref = index_ref
        (index_ref,) = take(1)
    x_all, index_here, even, odd, top_ref, sum_ref, found_ref = take(7)
    count = x_all.shape[0]
    width = weight_ref.shape[1]
    cuts = [0, width % TILE, *range(width % TILE + TILE, width, TILE), width - TILE // 2, width]
    edges = [(left, right) for left, right in zip(cuts, cuts[1:]) if left < right]
    if first:
        picks, tokens = picks_ref.shape
        for left in range(0, tokens, LANES):
            some = picks_ref[:, left : left + LANES]
            more = jnp.full((LANES - picks, LANES), -1, jnp.int32)
            index_ref[left : left + LANES, :] = jnp.concatenate([some, more], axis=0).T
    at = 0
    for x_ref in x_refs:
        x_all[at : at + x_ref.shape[0], :] = x_ref[...]
        at += x_ref.shape[0]
    block_rows = index_ref.shape[0] // (RING * RING * CORES)

    def rows_of(block):
        return pl.ds(pl.multiple_of(block_ref[0, block] * block_rows, block_rows), block_rows)

    start = lax.axis_index(AXIS) * width
    for b, block in enumerate(blocks):
        index_here[b * block_rows : (b + 1) * block_rows, :] = index_ref[rows_of(block), :] - start

    def fold(logits, tile, columns):
        for b in range(count // ROWS):
            rows = slice(b * ROWS, (b + 1) * ROWS)
            wanted = index_here[rows, :]
            wanted_tile = lax.shift_right_arithmetic(wanted, 7)
            wanted_lane = lax.bitwise_and(wanted, LANES - 1)
            parts = [logits[rows, j * LANES : (j + 1) * LANES] for j in range(columns)]
            top = functools.reduce(jnp.maximum, parts)
            if tile:
                before = top_ref[rows, :]
                top = jnp.maximum(before, top)
            total = functools.reduce(jnp.add, [jnp.exp(p - top) for p in parts])
            if tile:
                total = total + sum_ref[rows, :] * jnp.exp(before - top)
                found = found_ref[rows, :]
            else:
                found = jnp.zeros((ROWS, LANES), jnp.float32)
            for j, part in enumerate(parts):
                seen = jnp.take_along_axis(part, wanted_lane, axis=1, mode="promise_in_bounds")
                found = jnp.where(wanted_tile == tile + j, seen, found)
            top_ref[rows, :] = top
            sum_ref[rows, :] = total
            found_ref[rows, :] = found

    waiting = None
    for t, (left, right) in enumerate(edges):
        logits = (even, odd)[t % 2]
        logits[:, : right - left] = jnp.dot(
            x_all[...], weight_ref[:, left:right], preferred_element_type=jnp.float32
        )
        if waiting is not None:
            fold(*waiting)
        waiting = (logits, left // LANES, (right - left) // LANES)
    fold(*waiting)
    lane = lax.broadcasted_iota(jnp.int32, (ROWS, LANES), 1)
    rest = out_ref
    if last:
        held, rest = take(2)
    for b in range(count // ROWS):
        rows = slice(b * ROWS, (b + 1) * ROWS)
        tops = top_ref[rows, :]
        top = jnp.max(tops, axis=1, keepdims=True)
        total = jnp.sum(sum_ref[rows, :] * jnp.exp(tops - top), axis=1, keepdims=True)
        found = jnp.where(lane == LANES - 2, top, found_ref[rows, :])
        rest[rows, :] = jnp.where(lane == LANES - 1, total, found)
    if last:
        block = 0
        for held_ref in [*held_refs, rest]:
            for at in range(0, held_ref.shape[0], block_rows):
                held[rows_of(block), :] = held_ref[at : at + block_rows, :]
                block += 1
    if last:
        unroll = 16

        def move(b, _):
            for i in range(unroll):
                r = b * unroll + i
                out_ref[pl.ds(r, 1), :] = held[pl.ds(order_ref[r], 1), :]
            return 0

        lax.fori_loop(0, out_ref.shape[0] // unroll, move, 0)


def chunk(blocks, xs, members, held, weight, index, order=None, first=False):
    last = order is not None
    count = sum(x.shape[0] for x in xs)
    depth, width = weight.shape
    tokens = index.shape[1 if first else 0]
    scalar = pl.BlockSpec(memory_space=pltpu.SMEM)
    vector = pl.BlockSpec(memory_space=pltpu.VMEM)
    rows = pltpu.VMEM((count, LANES), jnp.float32)
    out_shape = [jax.ShapeDtypeStruct((tokens if last else count, LANES), jnp.float32)]
    scratch = [
        pltpu.VMEM((count, depth), jnp.bfloat16),
        pltpu.VMEM((count, LANES), jnp.int32),
        pltpu.VMEM((count, TILE), jnp.float32),
        pltpu.VMEM((count, TILE), jnp.float32),
        rows,
        rows,
        rows,
    ]
    if first:
        out_shape.append(jax.ShapeDtypeStruct((tokens, LANES), jnp.int32))
    if last:
        scratch += [pltpu.VMEM((tokens, LANES), jnp.float32), rows]
    out = pl.pallas_call(
        functools.partial(
            chunk_kernel,
            pieces=len(xs),
            blocks=members,
            ahead=len(held),
            first=first,
            last=last,
        ),
        out_shape=out_shape,
        in_specs=[scalar] * (2 if last else 1)
        + [vector] * (len(xs) + len(held) + 2),
        out_specs=[vector] * len(out_shape),
        scratch_shapes=scratch,
        compiler_params=pltpu.CompilerParams(vmem_limit_bytes=12 * 1024 * 1024),
        cost_estimate=pl.CostEstimate(
            flops=2 * count * depth * width,
            bytes_accessed=2 * depth * width,
            transcendentals=count * width,
        ),
    )(blocks, *([order] if last else []), *xs, *held, weight, index)
    return out if first else out[0]


def combine_kernel(rows_ref, logprobs_ref, log_total_ref):
    rows = rows_ref[...]
    shards, own, _ = rows.shape
    shifted = pltpu.roll(rows.reshape(shards * own, LANES), 1, 1).reshape(rows.shape)
    top = jnp.max(shifted, axis=0)
    total = jnp.sum(rows * jnp.exp(shifted - top[None]), axis=0)
    lane = lax.broadcasted_iota(jnp.int32, (own, LANES), 1)
    log_total = jnp.where(lane == LANES - 1, top + jnp.log(total), 0.0)
    log_total = jnp.sum(log_total, axis=1, keepdims=True)
    picks = logprobs_ref.shape[1]
    logprobs_ref[...] = jnp.sum(rows, axis=0)[:, :picks] - log_total
    row = lax.broadcasted_iota(jnp.int32, (own, LANES), 0)
    line = jnp.sum(jnp.where(row == lane, log_total, 0.0), axis=0, keepdims=True)
    log_total_ref[...] = line[:, :own]


def combine(rows, picks):
    own = rows.shape[1]
    vector = pl.BlockSpec(memory_space=pltpu.VMEM)
    logprobs, log_total = pl.pallas_call(
        combine_kernel,
        out_shape=[
            jax.ShapeDtypeStruct((own, picks), jnp.float32),
            jax.ShapeDtypeStruct((1, own), jnp.float32),
        ],
        in_specs=[vector],
        out_specs=[vector, vector],
        compiler_params=pltpu.CompilerParams(vmem_limit_bytes=4 * 1024 * 1024),
    )(rows)
    return logprobs, log_total.reshape(own)


def shifts(value, phase):
    received = []
    for k in STEPS[1:]:
        received.append(lax.ppermute(value, AXIS, along(k, phase)))
    return received


def program(hidden_states, head_weight, pick_index, owner_order):
    shard_count = lax.axis_size(AXIS)
    own_rows = hidden_states.shape[0]
    pick_count = pick_index.shape[1]
    swap = pairs(lambda x, z, c: (x, z, 1 - c))

    def swapped(value):
        return lax.ppermute(value, AXIS, swap)

    blocks = table()
    own = hidden_states
    line = jnp.concatenate(shifts(own, 0))
    cross = jnp.concatenate(shifts(own, 1))
    rest = shifts(line, 1)
    early = {"own": own, "line": line, "cross": cross}
    at = list(range(shard_count))
    sizes = [len(part) for part in arrivals()]
    cut = sizes[0], sizes[0] + sizes[1]
    others = [swapped(v) for v in early.values()]
    xs = [*early.values(), *others]
    first, index = chunk(blocks, xs, at[: cut[0]], [], head_weight, pick_index.T, first=True)
    *near, far = rest
    *near, first = lax.optimization_barrier((*near, first))
    others = [swapped(v) for v in near]
    second = chunk(blocks, near, at[cut[0] : cut[1]], [], head_weight, index)
    far, second = lax.optimization_barrier((far, second))
    xs = [far, *others, swapped(far)]
    held = [first, second]
    rows = chunk(blocks, xs, at[cut[1] :], held, head_weight, index, order=owner_order)
    rows = rows.reshape(shard_count, own_rows, LANES)
    received = lax.all_to_all(rows, AXIS, split_axis=0, concat_axis=0, tiled=True)
    return combine(received, pick_count)


def solution(mesh):
    in_specs = (P(("group", "vocab"), None), P(None, "vocab"), P("group", None), P("group"))
    out_specs = (P(("group", "vocab"), None), P(("group", "vocab")))
    return jax.shard_map(
        program, mesh=mesh, in_specs=in_specs, out_specs=out_specs, check_vma=False
    )
```

```python
import functools

import jax
import jax.numpy as jnp
from jax import lax
from jax.experimental import pallas as pl
from jax.experimental.pallas import tpu as pltpu
from jax.sharding import PartitionSpec as P


LANES = 128
ROWS = 8
RING = 4
CORES = 2
TILE = 512
AXIS = "vocab"
STEPS = (0, 1, 3, 2)
COVER_FLOPS = 1 << 35
EARLY = 2 * RING - 1
LATE = (RING - 1) ** 2


def index_of(x, z, core):
    return (x * RING + z) * CORES + core


def place_of(index):
    return index >> 3, (index >> 1) & 3, index & 1


def pairs(target):
    return [
        (index_of(x, z, c), index_of(*target(x, z, c)))
        for x in range(RING)
        for z in range(RING)
        for c in range(CORES)
    ]


def along(step, first_axis_core):
    return pairs(
        lambda x, z, c: ((x + step) % RING, z, c)
        if c == first_axis_core
        else (x, (z + step) % RING, c)
    )


def table_kernel(out_ref):
    x, z, c = place_of(lax.axis_index(AXIS))
    at = lax.broadcasted_iota(jnp.int32, out_ref.shape, 1)
    late = at - 2 * EARLY
    one = jnp.ones_like(at)
    other = jnp.where(at >= EARLY, one, 0) - jnp.where(late >= 0, one, 0) + jnp.where(late >= LATE, one, 0)
    soon = at - EARLY * other
    late = late - LATE * other
    turn = jnp.where(late >= RING - 1, one, 0) + jnp.where(late >= 2 * (RING - 1), one, 0)
    second = jnp.where(at < 2 * EARLY, jnp.maximum(soon - (RING - 1), 0), 1 + turn)
    first = jnp.where(soon >= RING, 0, soon)
    first = jnp.where(at < 2 * EARLY, first, 1 + late - (RING - 1) * turn)
    first, second = first ^ (first >> 1), second ^ (second >> 1)
    core = c ^ other
    from_x = (x - jnp.where(core == 0, first, second)) & 3
    from_z = (z - jnp.where(core == 0, second, first)) & 3
    out_ref[...] = index_of(from_x, from_z, core)


def table():
    return pl.pallas_call(
        table_kernel,
        out_shape=jax.ShapeDtypeStruct((1, LANES), jnp.int32),
        out_specs=pl.BlockSpec(memory_space=pltpu.VMEM),
        compiler_params=pltpu.CompilerParams(vmem_limit_bytes=1024 * 1024),
        cost_estimate=pl.CostEstimate(flops=COVER_FLOPS, bytes_accessed=1024, transcendentals=0),
    )()


def chunk_kernel(*refs, pieces, blocks, ahead, first, last):
    refs = list(refs)

    def take(n):
        taken, refs[:n] = refs[:n], []
        return taken

    (block_ref,) = take(1)
    if last:
        (order_ref,) = take(1)
    x_refs, held_refs = take(pieces), take(ahead)
    weight_ref, index_ref, out_ref = take(3)
    if first:
        picks_ref = index_ref
        (index_ref,) = take(1)
    x_all, index_here, even, odd, top_ref, sum_ref, found_ref = take(7)
    count = x_all.shape[0]
    width = weight_ref.shape[1]
    edges = [(left, min(left + TILE, width)) for left in range(0, width, TILE)]
    if first:
        picks, tokens = picks_ref.shape
        for left in range(0, tokens, LANES):
            some = picks_ref[:, left : left + LANES]
            more = jnp.full((LANES - picks, LANES), -1, jnp.int32)
            index_ref[left : left + LANES, :] = jnp.concatenate([some, more], axis=0).T
    if len(x_refs) == 1:
        x_all = x_refs[0]
    at = 0
    for x_ref in x_refs if len(x_refs) > 1 else ():
        x_all[at : at + x_ref.shape[0], :] = x_ref[...]
        at += x_ref.shape[0]
    block_rows = index_ref.shape[0] // (RING * RING * CORES)

    def rows_of(block):
        return pl.ds(pl.multiple_of(block_ref[0, block] * block_rows, block_rows), block_rows)

    start = lax.axis_index(AXIS) * width
    for b, block in enumerate(blocks):
        index_here[b * block_rows : (b + 1) * block_rows, :] = index_ref[rows_of(block), :] - start

    def fold(logits, tile, columns):
        for b in range(count // ROWS):
            rows = slice(b * ROWS, (b + 1) * ROWS)
            wanted = index_here[rows, :]
            wanted_tile = lax.shift_right_arithmetic(wanted, 7)
            wanted_lane = lax.bitwise_and(wanted, LANES - 1)
            parts = [logits[rows, j * LANES : (j + 1) * LANES] for j in range(columns)]
            top = functools.reduce(jnp.maximum, parts)
            if tile:
                before = top_ref[rows, :]
                top = jnp.maximum(before, top)
            total = functools.reduce(jnp.add, [jnp.exp(p - top) for p in parts])
            if tile:
                total = total + sum_ref[rows, :] * jnp.exp(before - top)
                found = found_ref[rows, :]
            else:
                found = jnp.zeros((ROWS, LANES), jnp.float32)
            for j, part in enumerate(parts):
                seen = jnp.take_along_axis(part, wanted_lane, axis=1, mode="promise_in_bounds")
                found = jnp.where(wanted_tile == tile + j, seen, found)
            top_ref[rows, :] = top
            sum_ref[rows, :] = total
            found_ref[rows, :] = found

    waiting = None
    for t, (left, right) in enumerate(edges):
        logits = (even, odd)[t % 2]
        logits[:, : right - left] = jnp.dot(
            x_all[...], weight_ref[:, left:right], preferred_element_type=jnp.float32
        )
        if waiting is not None:
            fold(*waiting)
        waiting = (logits, left // LANES, (right - left) // LANES)
    fold(*waiting)
    lane = lax.broadcasted_iota(jnp.int32, (ROWS, LANES), 1)
    rest = out_ref
    if last:
        held, rest = take(2)
    for b in range(count // ROWS):
        rows = slice(b * ROWS, (b + 1) * ROWS)
        tops = top_ref[rows, :]
        top = jnp.max(tops, axis=1, keepdims=True)
        total = jnp.sum(sum_ref[rows, :] * jnp.exp(tops - top), axis=1, keepdims=True)
        found = jnp.where(lane == LANES - 2, top, found_ref[rows, :])
        rest[rows, :] = jnp.where(lane == LANES - 1, total, found)
    if last:
        block = 0
        for held_ref in [*held_refs, rest]:
            for at in range(0, held_ref.shape[0], block_rows):
                held[rows_of(block), :] = held_ref[at : at + block_rows, :]
                block += 1
    if last:
        unroll = 16

        def move(b, _):
            for i in range(unroll):
                r = b * unroll + i
                out_ref[pl.ds(r, 1), :] = held[pl.ds(order_ref[r], 1), :]
            return 0

        lax.fori_loop(0, out_ref.shape[0] // unroll, move, 0)


def chunk(blocks, xs, members, held, weight, index, order=None, first=False):
    last = order is not None
    count = sum(x.shape[0] for x in xs)
    depth, width = weight.shape
    tokens = index.shape[1 if first else 0]
    scalar = pl.BlockSpec(memory_space=pltpu.SMEM)
    vector = pl.BlockSpec(memory_space=pltpu.VMEM)
    rows = pltpu.VMEM((count, LANES), jnp.float32)
    out_shape = [jax.ShapeDtypeStruct((tokens if last else count, LANES), jnp.float32)]
    scratch = [
        pltpu.VMEM((count, depth), jnp.bfloat16),
        pltpu.VMEM((count, LANES), jnp.int32),
        pltpu.VMEM((count, TILE), jnp.float32),
        pltpu.VMEM((count, TILE), jnp.float32),
        rows,
        rows,
        rows,
    ]
    if first:
        out_shape.append(jax.ShapeDtypeStruct((tokens, LANES), jnp.int32))
    if last:
        scratch += [pltpu.VMEM((tokens, LANES), jnp.float32), rows]
    out = pl.pallas_call(
        functools.partial(
            chunk_kernel,
            pieces=len(xs),
            blocks=members,
            ahead=len(held),
            first=first,
            last=last,
        ),
        out_shape=out_shape,
        in_specs=[scalar] * (2 if last else 1)
        + [vector] * (len(xs) + len(held) + 2),
        out_specs=[vector] * len(out_shape),
        scratch_shapes=scratch,
        compiler_params=pltpu.CompilerParams(vmem_limit_bytes=12 * 1024 * 1024),
        cost_estimate=pl.CostEstimate(
            flops=2 * count * depth * width,
            bytes_accessed=2 * depth * width,
            transcendentals=count * width,
        ),
    )(blocks, *([order] if last else []), *xs, *held, weight, index)
    return out if first else out[0]


def combine_kernel(rows_ref, logprobs_ref, log_total_ref):
    rows = rows_ref[...]
    shards, own, _ = rows.shape
    shifted = pltpu.roll(rows.reshape(shards * own, LANES), 1, 1).reshape(rows.shape)
    top = jnp.max(shifted, axis=0)
    total = jnp.sum(rows * jnp.exp(shifted - top[None]), axis=0)
    lane = lax.broadcasted_iota(jnp.int32, (own, LANES), 1)
    log_total = jnp.where(lane == LANES - 1, top + jnp.log(total), 0.0)
    log_total = jnp.sum(log_total, axis=1, keepdims=True)
    picks = logprobs_ref.shape[1]
    logprobs_ref[...] = jnp.sum(rows, axis=0)[:, :picks] - log_total
    row = lax.broadcasted_iota(jnp.int32, (own, LANES), 0)
    line = jnp.sum(jnp.where(row == lane, log_total, 0.0), axis=0, keepdims=True)
    log_total_ref[...] = line[:, :own]


def combine(rows, picks):
    own = rows.shape[1]
    vector = pl.BlockSpec(memory_space=pltpu.VMEM)
    logprobs, log_total = pl.pallas_call(
        combine_kernel,
        out_shape=[
            jax.ShapeDtypeStruct((own, picks), jnp.float32),
            jax.ShapeDtypeStruct((1, own), jnp.float32),
        ],
        in_specs=[vector],
        out_specs=[vector, vector],
        compiler_params=pltpu.CompilerParams(vmem_limit_bytes=4 * 1024 * 1024),
    )(rows)
    return logprobs, log_total.reshape(own)


def shifts(value, phase):
    received = []
    for k in STEPS[1:]:
        received.append(lax.ppermute(value, AXIS, along(k, phase)))
    return received


def program(hidden_states, head_weight, pick_index, owner_order):
    shard_count = lax.axis_size(AXIS)
    own_rows = hidden_states.shape[0]
    pick_count = pick_index.shape[1]
    swap = pairs(lambda x, z, c: (x, z, 1 - c))

    def swapped(value):
        return lax.ppermute(value, AXIS, swap)

    blocks = table()
    own = hidden_states
    line = jnp.concatenate(shifts(own, 0))
    cross = jnp.concatenate(shifts(own, 1))
    rest = shifts(line, 1)
    early = {"own": own, "line": line, "cross": cross}
    at = list(range(shard_count))
    cut = 2 * EARLY, 2 * EARLY + LATE
    others = [swapped(v) for v in early.values()]
    xs = [jnp.concatenate([*early.values(), *others])]
    first, index = chunk(blocks, xs, at[: cut[0]], [], head_weight, pick_index.T, first=True)
    *rest, first = lax.optimization_barrier((*rest, first))
    late = jnp.concatenate(rest)
    second = chunk(blocks, [late], at[cut[0] : cut[1]], [], head_weight, index)
    others = swapped(late)
    held = [first, second]
    rows = chunk(blocks, [others], at[cut[1] :], held, head_weight, index, order=owner_order)
    rows = rows.reshape(shard_count, own_rows, LANES)
    received = lax.all_to_all(rows, AXIS, split_axis=0, concat_axis=0, tiled=True)
    return combine(received, pick_count)


def solution(mesh):
    in_specs = (P(("group", "vocab"), None), P(None, "vocab"), P("group", None), P("group"))
    out_specs = (P(("group", "vocab"), None), P(("group", "vocab")))
    return jax.shard_map(
        program, mesh=mesh, in_specs=in_specs, out_specs=out_specs, check_vma=False
    )
```
